32 devices in a mesh: site: 8 (over z, x), clade: 4 (over y, core).
Axes of the slice: x: 2, y: 2, z: 4, core: 2. Of those that a mesh axis runs over, the one named last changes fastest.
Arguments:
- tips: int32 [128, 32768], P('clade', 'site'), may hold values from 0 to 4
- transition: float32 [248, 4, 4, 4], P('clade'), may hold values from 0 to 1, as said below
- clade_children: int32 [124, 2], P('clade'), may hold values from 0 to 61, as said below
- upper_transition: float32 [6, 4, 4, 4], replicated, may hold values from 0 to 1, as said below
- upper_children: int32 [3, 2], replicated, may hold values from 0 to 5, as said below
- pattern_weights: int32 [32768], P('site'), may hold values from 1 to 8
Outputs:
- weighted_loglik: float32 [32768], P(('site', 'clade'))
- mean_loglik: float32 [], replicated
The draws below stay inside these ranges and needn't reach their ends.
Inputs may be any that keep to these rules, and one draw needn't show every extreme that they name: `tips`: code 4 marks a gap or an unknown base. `transition`: every row of every 4 x 4 block is positive and sums to 1. `upper_transition`: every row of every 4 x 4 block is positive and sums to 1. `clade_children`: rows k * (31) to (k + 1) * 31 - 1 belong to clade k; its row j holds two different node numbers below 32 + j, and each node 0 to 61 of the clade is a child in exactly one row of the clade. `upper_children`: row j holds two different node numbers below 4 + j, and each node 0 to 5 is a child in exactly one row.
All inputs are finite; a program needn't handle non-finite values.
Results may differ from the reference program's by a relative error of at most 0.0003.
Values sent between devices are 32-bit elements; how exact they have to be, the bound alone decides.
A program may use at most 64 MiB of HBM per device.

```python
import jax
import jax.numpy as jnp
from jax import lax

LEAF = 32
RATES = 4
TAXA = 128
SITES = 32768
N_CLADE = 4


def tree_merges(base_key, leaf_count):
    active = jnp.arange(leaf_count, dtype=jnp.int32)
    merges = jnp.zeros((leaf_count - 1, 2), jnp.int32)

    def advance(node_index, state_pair):
        active_now, merges_now = state_pair
        live_count = leaf_count - node_index
        step_key = jax.random.fold_in(base_key, node_index)
        key_one, key_two = jax.random.split(step_key)
        first_pick = jax.random.randint(key_one, (), 0, live_count)
        second_pick = jax.random.randint(key_two, (), 0, live_count - 1)
        second_pick = jnp.where(second_pick >= first_pick, second_pick + 1, second_pick)
        pair_row = jnp.stack([active_now[first_pick], active_now[second_pick]]).astype(jnp.int32)
        merges_now = merges_now.at[node_index].set(pair_row)
        active_now = active_now.at[first_pick].set((leaf_count + node_index).astype(jnp.int32))
        active_now = active_now.at[second_pick].set(active_now[live_count - 1])
        return (active_now, merges_now)
    return lax.fori_loop(0, leaf_count - 1, advance, (active, merges))[1]


def stochastic(base_key, edge_count):
    key_one, key_two = jax.random.split(base_key)
    lengths = jnp.exp(jax.random.uniform(key_one, (edge_count, RATES, 1, 1), jnp.float32, jnp.log(0.03), jnp.log(0.6)))
    roughness = jax.random.uniform(key_two, (edge_count, RATES, 4, 4), jnp.float32, 0.3, 1.0)
    identity = jnp.eye(4, dtype=jnp.float32)
    raw_rates = identity + lengths * roughness * (1.0 - identity)
    return raw_rates / jnp.sum(raw_rates, axis=-1, keepdims=True)


def draw_transition(key, part):
    return stochastic(jax.random.fold_in(key, 21), (2 * LEAF - 2) * N_CLADE)


def draw_upper_transition(key, part):
    return stochastic(jax.random.fold_in(key, 22), 2 * N_CLADE - 2)


def draw_clade_children(key, part):
    clade_keys = jax.random.split(jax.random.fold_in(key, 11), N_CLADE)
    merged = jax.vmap(lambda subkey: tree_merges(subkey, LEAF))(clade_keys)
    return merged.reshape((N_CLADE * (LEAF - 1), 2))


def draw_upper_children(key, part):
    return tree_merges(jax.random.fold_in(key, 12), N_CLADE)


def plant(array, rng, least, top_value):
    place = [jax.random.randint(jax.random.fold_in(rng, axis), (), 0, length) for axis, length in enumerate(array.shape)]
    widest = array.shape.index(max(array.shape))
    next_to = place[:widest] + [(place[widest] + 1) % array.shape[widest]] + place[widest + 1:]
    return array.at[tuple(place)].set(least).at[tuple(next_to)].set(top_value)


def setup_inputs(seed: int = 0) -> dict:
    arg_keys = jax.random.split(jax.random.key(seed), 7)
    return {
        "tips": plant(jax.random.randint(arg_keys[0], (TAXA, SITES), 0, 5), jax.random.fold_in(arg_keys[0], 1), 0, 4).astype(jnp.int32),
        "transition": draw_transition(jax.random.fold_in(arg_keys[6], 71), 0),
        "clade_children": draw_clade_children(jax.random.fold_in(arg_keys[6], 71), 0),
        "upper_transition": draw_upper_transition(jax.random.fold_in(arg_keys[6], 71), 0),
        "upper_children": draw_upper_children(jax.random.fold_in(arg_keys[6], 71), 0),
        "pattern_weights": plant(jax.random.randint(arg_keys[5], (SITES,), 1, 9), jax.random.fold_in(arg_keys[5], 1), 1, 8).astype(jnp.int32),
    }


def transform(matrix, values_in):
    return jnp.einsum("rab,rbs->ras", matrix, values_in, precision=lax.Precision.HIGHEST)


def prune_tree(partials, scales, matrices, merges, first_new):
    def advance(node_index, state_pair):
        cur_parts, cur_scales = state_pair
        left_index = merges[node_index, 0]
        right_index = merges[node_index, 1]
        product = transform(matrices[left_index], cur_parts[left_index]) * transform(matrices[right_index], cur_parts[right_index])
        biggest = jnp.max(product, axis=(0, 1))
        new_scale = cur_scales[left_index] + cur_scales[right_index] + jnp.log(biggest)
        target = (first_new + node_index).astype(jnp.int32)
        cur_parts = lax.dynamic_update_index_in_dim(cur_parts, product / biggest, target, 0)
        cur_scales = lax.dynamic_update_index_in_dim(cur_scales, new_scale, target, 0)
        return cur_parts, cur_scales

    return lax.fori_loop(0, merges.shape[0], advance, (partials, scales))


def tip_partials(tip_codes, rate_count):
    states = jnp.arange(4, dtype=jnp.int32)
    matches = (tip_codes[:, None, :] == states[None, :, None]) | (tip_codes[:, None, :] == 4)
    single = matches.astype(jnp.float32)
    return jnp.broadcast_to(single[:, None], (single.shape[0], rate_count, 4, single.shape[2]))


def clade_root(tip_codes, matrices, merges):
    leaf_count = tip_codes.shape[0]
    site_count = tip_codes.shape[1]
    rate_count = matrices.shape[1]
    leaves = tip_partials(tip_codes, rate_count)
    partials = jnp.concatenate([leaves, jnp.zeros((leaf_count - 1, rate_count, 4, site_count), jnp.float32)], axis=0)
    scales = jnp.zeros((2 * leaf_count - 1, site_count), jnp.float32)
    partials, scales = prune_tree(partials, scales, matrices, merges, leaf_count)
    return partials[-1], scales[-1]


def upper_root(root_parts, root_scales, matrices, merges):
    clade_total = root_parts.shape[0]
    partials = jnp.concatenate([root_parts, jnp.zeros((clade_total - 1,) + root_parts.shape[1:], jnp.float32)], axis=0)
    scales = jnp.concatenate([root_scales, jnp.zeros((clade_total - 1, root_scales.shape[1]), jnp.float32)], axis=0)
    partials, scales = prune_tree(partials, scales, matrices, merges, clade_total)
    return partials[-1], scales[-1]


def site_loglik(root_part, root_scale, weights, taxa_total):
    summed = jnp.sum(root_part, axis=(0, 1)) / (4.0 * root_part.shape[0])
    return weights.astype(jnp.float32) * (jnp.log(summed) + root_scale) / taxa_total


def reference(tips, transition, clade_children, upper_transition, upper_children, pattern_weights):
    edge_count = 2 * LEAF - 2

    def one_clade(clade_index):
        tip_codes = lax.dynamic_slice_in_dim(tips, clade_index * LEAF, LEAF, 0)
        matrices = lax.dynamic_slice_in_dim(transition, clade_index * edge_count, edge_count, 0)
        merges = lax.dynamic_slice_in_dim(clade_children, clade_index * (LEAF - 1), LEAF - 1, 0)
        return clade_root(tip_codes, matrices, merges)

    root_parts, root_scales = lax.map(one_clade, jnp.arange(N_CLADE, dtype=jnp.int32))
    final_part, final_scale = upper_root(root_parts, root_scales, upper_transition, upper_children)
    weighted = site_loglik(final_part, final_scale, pattern_weights, float(LEAF * N_CLADE))
    return weighted, jnp.sum(weighted) / SITES
```

```python
import functools

import jax
import jax.numpy as jnp
from jax import lax
from jax.experimental import pallas as pl
from jax.experimental.pallas import tpu as pltpu
from jax.sharding import PartitionSpec as P

MESH = pl.DeviceIdType.MESH


def tree_max(values):
    while len(values) > 1:
        paired = [jnp.maximum(a, b) for a, b in zip(values[::2], values[1::2])]
        values = paired + ([values[-1]] if len(values) % 2 else [])
    return values[0]


def tree_sum(values):
    while len(values) > 1:
        paired = [a + b for a, b in zip(values[::2], values[1::2])]
        values = paired + ([values[-1]] if len(values) % 2 else [])
    return values[0]


def kernel(dims, tips_in, matrices_in, children_in, upper_in, upper_children_in, weights_in,
           weighted, mean, tips, matrices, children, upper, upper_children, weights, load, branch, row_sum, upper_branch, moved, root, held,
           sums, root_send, root_recv, sum_send, sum_recv):
    leaves, rates, rows, clades, sites_axis = dims
    entries = rates * 4
    size = entries * 4
    inner = leaves - 1
    piece = rows // clades
    half_clades = clades // 2
    half_rows = rows // 2
    width = half_rows // 8
    me = lax.axis_index("clade")
    block = lax.axis_index("site")
    my_half = me // half_clades
    my_low = me % half_clades

    def tips_copy(turn):
        half = lax.rem(my_half + 1 + turn, 2)
        return pltpu.make_async_copy(
            tips_in.at[:, pl.ds(half * (half_rows * 8), half_rows * 8), :], tips.at[turn], load.at[turn])

    loads = [pltpu.make_async_copy(source, target, load.at[2 + k]) for k, (source, target) in enumerate([
        (matrices_in, matrices), (upper_in, upper), (children_in, children),
        (upper_children_in, upper_children), (weights_in, weights)])]
    loads[0].start()
    tips_copy(0).start()
    for copy in loads[1:]:
        copy.start()
    tips_copy(1).start()

    barrier = pltpu.get_barrier_semaphore()
    devices = clades * sites_axis
    mine = block * clades + me

    def greet(step, carry):
        other = lax.rem(mine + step, devices)
        pl.semaphore_signal(barrier, inc=1, device_id={"site": other // clades, "clade": lax.rem(other, clades)},
                            device_id_type=MESH)
        return carry

    lax.fori_loop(1, devices, greet, 0)

    def lay_out(node):
        branch[node * size:(node + 1) * size, :] = jnp.broadcast_to(matrices[:, node:node + 1], (size, 128))

    loads[0].wait()
    totals = tree_sum([matrices[pl.ds(b, entries, stride=4), :] for b in range(4)])
    def lay_out_tip(node):
        lay_out(node)
        row_sum[node * entries:(node + 1) * entries, :] = jnp.broadcast_to(totals[:, node:node + 1], (entries, 128))
    loads[1].wait()
    for node in range(2 * clades - 2):
        upper_branch[node * size:(node + 1) * size, :] = jnp.broadcast_to(upper[:, node:node + 1], (size, 128))

    def spread(ref, row, count=8):
        return jnp.broadcast_to(ref[pl.ds(row, 1), :], (count, 128))

    def merge(left, right):
        product = [a * b for a, b in zip(left, right)]
        biggest = tree_max(product)
        inverse = 1.0 / biggest
        return [p * inverse for p in product], jnp.log(biggest)

    def transform(ref, base, parts, store):
        count = parts[0][0].shape[0]
        for rate in range(rates):
            for state in range(4):
                entry = rate * 4 + state
                acc = None
                for b in range(4):
                    weight = spread(ref, base + entry * 4 + b, count)
                    terms = [weight * part[rate * 4 + b] for part in parts]
                    acc = terms if acc is None else [x + y for x, y in zip(acc, terms)]
                for w, value in enumerate(acc):
                    store(entry, w, value)

    root_copies = []
    for turn in range(2):
        half = lax.rem(my_half + 1 + turn, 2)

        def tip(i, carry):
            codes = [tips[turn, i // 8, pl.ds(w * 64 + i % 8, 8, stride=8), :] for w in range(width)]
            is_code = [[code == b for b in range(4)] for code in codes]
            for entry in range(entries):
                probs = [spread(branch, i * size + entry * 4 + b) for b in range(4)]
                total = spread(row_sum, i * entries + entry)
                for w in range(width):
                    value = total
                    for b in range(4):
                        value = jnp.where(is_code[w][b], probs[b], value)
                    moved[i * entries + entry, w * 8:(w + 1) * 8, :] = value
            return carry

        tips_copy(turn).wait()
        if turn == 0:
            for i in range(2):
                lay_out_tip(i)
            for i in range(leaves):
                if i + 2 < leaves:
                    lay_out_tip(i + 2)
                if i < inner - 1:
                    lay_out(leaves + i)
                tip(i, 0)
            for copy in loads[2:]:
                copy.wait()
        else:
            lax.fori_loop(0, leaves, tip, 0, unroll=2)

        def merged(j, scale):
            c = children[0, j]
            d = children[1, j]
            parts, scales = [], []
            for w in range(width):
                window = slice(w * 8, (w + 1) * 8)
                part, log_m = merge([moved[c * entries + e, window, :] for e in range(entries)],
                                    [moved[d * entries + e, window, :] for e in range(entries)])
                parts.append(part)
                scales.append(scale[w] + log_m)
            return parts, tuple(scales)

        def advance(j, scale):
            parts, scale = merged(j, scale)
            node = leaves + j

            def store(entry, w, value):
                moved[node * entries + entry, w * 8:(w + 1) * 8, :] = value

            transform(branch, node * size, parts, store)
            return scale

        scale = tuple(jnp.zeros((8, 128), jnp.float32) for _ in range(width))
        scale = lax.fori_loop(0, inner - 1, advance, scale)
        parts, scale = merged(inner - 1, scale)
        first = half * half_clades

        def store_root(entry, w, value):
            for k in range(8 // piece if piece < 8 else 1):
                row = w * 8 + k * piece
                if piece >= 8:
                    root[first + row // piece, entry, row % piece:row % piece + 8, :] = value
                else:
                    root[first + row // piece, entry, :, :] = value[k * piece:(k + 1) * piece, :]

        transform(upper_branch, me * size, parts, store_root)
        for w in range(width):
            store_root(entries, w, scale[w])

        if turn == 0:
            pl.semaphore_wait(barrier, devices - 1)
        for step in range(turn, half_clades):
            target = half * half_clades + lax.rem(my_low + step, half_clades)
            slot = turn * half_clades + step
            copy = pltpu.make_async_remote_copy(
                src_ref=root.at[target], dst_ref=held.at[me],
                send_sem=root_send.at[slot], recv_sem=root_recv.at[slot],
                device_id={"clade": target}, device_id_type=MESH)
            copy.start()
            root_copies.append(copy)

    held[me] = root[me]
    for copy in root_copies:
        copy.wait_recv()

    scale = tree_sum([held[k, entries] for k in range(clades)])
    for j in range(clades - 1):
        c = upper_children[0, j]
        d = upper_children[1, j]
        part, log_m = merge([held[c, e] for e in range(entries)], [held[d, e] for e in range(entries)])
        scale = scale + log_m
        if j < clades - 2:
            def store_upper(entry, w, value):
                held[clades + j, entry, :, :] = value

            transform(upper_branch, (clades + j) * size, [part], store_upper)
    summed = tree_sum(part) / (4.0 * rates)
    value = weights[me].astype(jnp.float32) * (jnp.log(summed) + scale) / float(leaves * clades)
    weighted[...] = value

    sums[mine] = jnp.sum(value, axis=0, keepdims=True)

    def send_sum(step, carry):
        other = lax.rem(mine + step, devices)
        pltpu.make_async_remote_copy(
            src_ref=sums.at[mine], dst_ref=sums.at[mine], send_sem=sum_send, recv_sem=sum_recv,
            device_id={"site": other // clades, "clade": lax.rem(other, clades)}, device_id_type=MESH).start()
        return carry

    lax.fori_loop(1, devices, send_sum, 0)
    everyone = pltpu.make_async_remote_copy(
        src_ref=sums.at[pl.ds(1, devices - 1)], dst_ref=sums.at[pl.ds(1, devices - 1)],
        send_sem=sum_send, recv_sem=sum_recv, device_id={"clade": lax.rem(me + 1, clades)}, device_id_type=MESH)
    everyone.wait_recv()
    mean[...] = tree_sum([sums[k] for k in range(devices)])
    everyone.wait_send()
    for copy in root_copies:
        copy.wait_send()


def finish(sites, value, total, weighted, mean, sem):
    copy = pltpu.make_async_copy(value, weighted, sem)
    copy.start()
    mean[0] = jnp.sum(total[...]) / sites
    copy.wait()


def per_device(tips, transition, clade_children, upper_transition, upper_children, pattern_weights):
    leaves, sites = tips.shape
    rates = transition.shape[1]
    clades = lax.axis_size("clade")
    sites_axis = lax.axis_size("site")
    rows = sites // 128
    piece = rows // clades
    entries = rates * 4
    size = entries * 4
    nodes = 2 * leaves - 2
    codes = tips.reshape(leaves // 8, 8, rows, 128).transpose(0, 2, 1, 3).reshape(leaves // 8, rows * 8, 128)
    matrices = transition.transpose(1, 2, 3, 0).reshape(size, nodes)
    upper = upper_transition.transpose(1, 2, 3, 0).reshape(size, 2 * clades - 2)
    vmem = pl.BlockSpec(memory_space=pltpu.VMEM)
    smem = pl.BlockSpec(memory_space=pltpu.SMEM)
    weighted, mean = pl.pallas_call(
        functools.partial(kernel, (leaves, rates, rows, clades, sites_axis)),
        out_shape=(pltpu.VMEM((piece, 128), jnp.float32), pltpu.VMEM((1, 128), jnp.float32)),
        in_specs=[pl.BlockSpec(memory_space=pltpu.HBM)] * 6,
        out_specs=(vmem, vmem),
        scratch_shapes=[
            pltpu.VMEM((2, leaves // 8, rows * 4, 128), jnp.int32),
            pltpu.VMEM((size, nodes), jnp.float32),
            pltpu.SMEM((2, leaves - 1), jnp.int32),
            pltpu.VMEM((size, 2 * clades - 2), jnp.float32),
            pltpu.SMEM((2, clades - 1), jnp.int32),
            pltpu.VMEM((clades, piece, 128), jnp.int32),
            pltpu.SemaphoreType.DMA((7,)),
            pltpu.VMEM((nodes * size, 128), jnp.float32),
            pltpu.VMEM((leaves * entries, 128), jnp.float32),
            pltpu.VMEM(((2 * clades - 2) * size, 128), jnp.float32),
            pltpu.VMEM((nodes * entries, rows // 2, 128), jnp.float32),
            pltpu.VMEM((clades, entries + 1, piece, 128), jnp.float32),
            pltpu.VMEM((2 * clades - 2, entries + 1, piece, 128), jnp.float32),
            pltpu.VMEM((clades * sites_axis, 1, 128), jnp.float32),
            pltpu.SemaphoreType.DMA((clades,)),
            pltpu.SemaphoreType.DMA((clades,)),
            pltpu.SemaphoreType.DMA,
            pltpu.SemaphoreType.DMA,
        ],
        compiler_params=pltpu.CompilerParams(
            collective_id=0, has_side_effects=True, vmem_limit_bytes=67043328 - 16384),
    )(codes, matrices, clade_children.T, upper, upper_children.T, pattern_weights.reshape(clades, piece, 128))
    weighted, mean = pl.pallas_call(
        functools.partial(finish, float(sites * sites_axis)),
        out_shape=(jax.ShapeDtypeStruct((piece, 128), jnp.float32), jax.ShapeDtypeStruct((1,), jnp.float32)),
        in_specs=[vmem, vmem],
        out_specs=(pl.BlockSpec(memory_space=pltpu.HBM), smem),
        scratch_shapes=[pltpu.SemaphoreType.DMA],
    )(pltpu.with_memory_space_constraint(weighted, pltpu.VMEM), pltpu.with_memory_space_constraint(mean, pltpu.VMEM))
    return weighted.reshape(sites // clades), mean.reshape(())


def solution(mesh):
    placed = (
        P("clade", "site"),
        P("clade", None, None, None),
        P("clade", None),
        P(),
        P(),
        P("site"),
    )
    return jax.shard_map(
        per_device,
        mesh=mesh,
        in_specs=placed,
        out_specs=(P(("site", "clade")), P()),
        check_vma=False,
    )
```

```python
import functools

import jax
import jax.numpy as jnp
from jax import lax
from jax.experimental import pallas as pl
from jax.experimental.pallas import tpu as pltpu
from jax.sharding import PartitionSpec as P

MESH = pl.DeviceIdType.MESH
UNROLL = True
EARLY = 10
LATER = [[1], [2], []]


def tree_max(values):
    while len(values) > 1:
        paired = [jnp.maximum(a, b) for a, b in zip(values[::2], values[1::2])]
        values = paired + ([values[-1]] if len(values) % 2 else [])
    return values[0]


def tree_sum(values):
    while len(values) > 1:
        paired = [a + b for a, b in zip(values[::2], values[1::2])]
        values = paired + ([values[-1]] if len(values) % 2 else [])
    return values[0]


def look_up(table, code):
    dims = lax.GatherDimensionNumbers(
        offset_dims=(), collapsed_slice_dims=(0,), start_index_map=(0,),
        operand_batching_dims=(1,), start_indices_batching_dims=(1,))
    return lax.gather(table, code[..., None], dims, slice_sizes=(1, 1), mode=lax.GatherScatterMode.PROMISE_IN_BOUNDS)


def kernel(dims, tips_in, matrices_in, children_in, upper_in, upper_children_in, weights_in,
           weighted, mean, tips, matrices, children, upper, upper_children, weights, load,
           tables, branch, upper_branch, root, held, sums,
           root_send, root_recv, sum_send, sum_recv, here, *moved):
    leaves, rates, rows, clades, sites_axis = dims
    entries = rates * 4
    size = entries * 4
    nodes = 2 * leaves - 2
    inner = leaves - 1
    piece = rows // clades
    shares = 8 // piece
    windows = rows // 8
    near = windows // 2
    me = lax.axis_index("clade")
    block = lax.axis_index("site")
    devices = clades * sites_axis
    mine = block * clades + me
    own = me // shares
    my_share = lax.rem(me, shares)
    half, low = own // near, lax.rem(own, near)
    order = [(1 - half) * near + lax.rem(low + s, near) for s in range(near)]
    order += [half * near + lax.rem(low + s + 1, near) for s in range(near)]
    groups = [[t] for t in range(near)] + [list(range(near, windows))]

    def tips_start(turn):
        for k in range(leaves // 8):
            pltpu.make_async_copy(tips_in.at[k, pl.ds(order[turn] * 64, 64), :], tips.at[turn, k],
                                  load.at[0 if turn == 0 else 1]).start()

    def tips_wait(start, stop):
        span = tips.at[pl.ds(start, stop - start)]
        pltpu.make_async_copy(span, span, load.at[0 if start == 0 else 1]).wait()

    loads = [pltpu.make_async_copy(source, target, load.at[2 + k]) for k, (source, target) in enumerate([
        (matrices_in, matrices), (children_in, children), (upper_in, upper),
        (upper_children_in, upper_children), (weights_in, weights)])]
    loads[0].start()
    tips_start(0)
    for copy in loads[1:]:
        copy.start()
    for turn in range(1, windows):
        tips_start(turn)

    barrier = pltpu.get_barrier_semaphore()

    def to_site(index):
        return {"site": index // clades, "clade": lax.rem(index, clades)}

    for step in range(1, clades):
        pl.semaphore_signal(barrier, inc=1, device_id={"clade": lax.rem(me + step, clades)}, device_id_type=MESH)

    def greet(other, carry):
        pl.semaphore_signal(barrier, inc=1, device_id=to_site(other), device_id_type=MESH)
        return carry

    lax.fori_loop((block + 1) * clades, devices, greet, 0)

    loads[0].wait()
    first = lax.broadcasted_iota(jnp.int32, (8, 128), 0) < 4

    def lay_out(node):
        branch[node * size:(node + 1) * size, :] = jnp.broadcast_to(
            matrices[:, leaves + node:leaves + node + 1], (size, 128))

    def tip_codes(turn, i):
        return tips[turn, i // 8, pl.ds(lax.rem(i, 8), 8, stride=8), :]

    def tip_rest(i, targets):
        codes = {turn: tip_codes(turn, i) for group in targets for turn in groups[group]}
        for entry in range(entries):
            table = tables[i * entries + entry]
            for group in targets:
                for w, turn in enumerate(groups[group]):
                    moved[group][i * entries + entry, w * 8:(w + 1) * 8, :] = look_up(table, codes[turn])

    def tip_tables(i):
        for pair in range(entries // 2):
            both = jnp.broadcast_to(matrices[pair * 8:pair * 8 + 8, i:i + 1], (8, 128))
            tables[i * entries + 2 * pair] = jnp.where(first, both, 1.0)
            tables[i * entries + 2 * pair + 1] = jnp.where(first, pltpu.roll(both, 4, 0), 1.0)

    for i in range(EARLY):
        tip_tables(i)
    tips_wait(0, 1)
    for i in range(leaves):
        if i + EARLY < leaves:
            tip_tables(i + EARLY)
        tip_rest(i, [0])
        if not UNROLL and i < inner - 1:
            lay_out(i)
    loads[1].wait()
    tips_wait(1, windows)
    loads[2].wait()
    for node in range(2 * clades - 2):
        upper_branch[node * size:(node + 1) * size, :] = jnp.broadcast_to(upper[:, node:node + 1], (size, 128))

    def spread(ref, row, count=8):
        return jnp.broadcast_to(ref[pl.ds(row, 1), :], (count, 128))

    def merge(left, right):
        product = [a * b for a, b in zip(left, right)]
        biggest = tree_max(product)
        inverse = 1.0 / biggest
        return [p * inverse for p in product], jnp.log(biggest)

    def transform(ref, base, parts, store):
        count = parts[0][0].shape[0]
        for rate in range(rates):
            for state in range(4):
                entry = rate * 4 + state
                acc = None
                for b in range(4):
                    weight = spread(ref, base + entry * 4 + b, count)
                    terms = [weight * part[rate * 4 + b] for part in parts]
                    acc = terms if acc is None else [x + y for x, y in zip(acc, terms)]
                for w, value in enumerate(acc):
                    store(entry, w, value)

    def rows_of(j):
        return children[0, j] * entries, children[1, j] * entries

    for index, (group, target) in enumerate(zip(groups, moved)):
        width = len(group)

        def merged(c, d, scale):
            parts, scales = [], []
            for w in range(width):
                window = slice(w * 8, (w + 1) * 8)
                part, log_m = merge([target[c + e, window, :] for e in range(entries)],
                                    [target[d + e, window, :] for e in range(entries)])
                parts.append(part)
                scales.append(scale[w] + log_m)
            return parts, tuple(scales)

        def advance(j, carry):
            c, d, scale = carry
            after = rows_of(j + 1)
            if UNROLL and index == 0:
                lay_out(j)
            parts, scale = merged(c, d, scale)

            def store(entry, w, value):
                target[(leaves + j) * entries + entry, w * 8:(w + 1) * 8, :] = value

            transform(branch, j * size, parts, store)
            if later:
                tip_rest(j + leaves - inner + 1, later)
            return *after, scale

        later = LATER[index]
        if later:
            for i in range(leaves - inner + 1):
                tip_rest(i, later)
        carry = *rows_of(0), tuple(jnp.zeros((8, 128), jnp.float32) for _ in group)
        if UNROLL and index == 0:
            for j in range(inner - 1):
                carry = advance(j, carry)
        else:
            carry = lax.fori_loop(0, inner - 1, advance, carry)
        parts, scale = merged(*carry)

        def store_root(entry, w, value):
            for k in range(shares):
                root[group[w], k, entry] = value[k * piece:(k + 1) * piece, :]

        transform(upper_branch, me * size, parts, store_root)
        for w in range(width):
            store_root(entries, w, scale[w])

        if index == 0:
            pl.semaphore_wait(barrier, clades - 1 + block * clades)
        for turn in group:
            for k in range(shares):
                if turn < windows - 1:
                    share = k
                elif k:
                    share = lax.rem(my_share + k, shares)
                else:
                    continue
                pltpu.make_async_remote_copy(
                    src_ref=root.at[turn, share], dst_ref=held.at[me], send_sem=root_send, recv_sem=root_recv,
                    device_id={"clade": order[turn] * shares + share}, device_id_type=MESH).start()
        if index == len(groups) - 2:
            def answer(other, carry):
                pl.semaphore_signal(here, inc=1, device_id={"site": other}, device_id_type=MESH)
                return carry

            lax.fori_loop(0, block, answer, 0)

    held[me] = root[windows - 1, my_share]
    roots = pltpu.make_async_remote_copy(
        src_ref=held.at[pl.ds(0, clades - 1)], dst_ref=held.at[pl.ds(0, clades - 1)],
        send_sem=root_send, recv_sem=root_recv, device_id={"clade": lax.rem(me + 1, clades)}, device_id_type=MESH)
    loads[3].wait()
    loads[4].wait()
    roots.wait_recv()

    scale = tree_sum([held[k, entries] for k in range(clades)])
    for j in range(clades - 1):
        c = upper_children[0, j]
        d = upper_children[1, j]
        part, log_m = merge([held[c, e] for e in range(entries)], [held[d, e] for e in range(entries)])
        scale = scale + log_m
        if j < clades - 2:
            def store_upper(entry, w, value):
                held[clades + j, entry, :, :] = value

            transform(upper_branch, (clades + j) * size, [part], store_upper)
    summed = tree_sum(part) / (4.0 * rates)
    value = weights[me].astype(jnp.float32) * (jnp.log(summed) + scale) / float(leaves * clades)
    weighted[...] = value

    sums[mine] = jnp.sum(value, axis=0, keepdims=True)

    def send_sum(other, carry):
        pltpu.make_async_remote_copy(
            src_ref=sums.at[mine], dst_ref=sums.at[mine], send_sem=sum_send, recv_sem=sum_recv,
            device_id=to_site(other), device_id_type=MESH).start()
        return carry

    lax.fori_loop(0, block * clades, send_sum, 0)
    for step in range(1, clades):
        send_sum(block * clades + lax.rem(me + step, clades), 0)

    @pl.when(block < sites_axis - 1)
    def _():
        pl.semaphore_wait(here, sites_axis - 1 - block)

    lax.fori_loop((block + 1) * clades, devices, send_sum, 0)
    everyone = pltpu.make_async_remote_copy(
        src_ref=sums.at[pl.ds(1, devices - 1)], dst_ref=sums.at[pl.ds(1, devices - 1)],
        send_sem=sum_send, recv_sem=sum_recv, device_id={"clade": lax.rem(me + 1, clades)}, device_id_type=MESH)
    roots.wait_send()
    everyone.wait_send()
    everyone.wait_recv()
    mean[...] = tree_sum([sums[k] for k in range(devices)])


def finish(sites, value, total, weighted, mean, sem):
    copy = pltpu.make_async_copy(value, weighted, sem)
    copy.start()
    mean[0] = jnp.sum(total[...]) / sites
    copy.wait()


def per_device(tips, transition, clade_children, upper_transition, upper_children, pattern_weights):
    leaves, sites = tips.shape
    rates = transition.shape[1]
    clades = lax.axis_size("clade")
    sites_axis = lax.axis_size("site")
    rows = sites // 128
    piece = rows // clades
    windows = rows // 8
    near = windows // 2
    entries = rates * 4
    size = entries * 4
    nodes = 2 * leaves - 2
    codes = tips.reshape(leaves // 8, 8, rows, 128).transpose(0, 2, 1, 3).reshape(leaves // 8, rows * 8, 128)
    matrices = transition.transpose(1, 2, 3, 0).reshape(size, nodes)
    upper = upper_transition.transpose(1, 2, 3, 0).reshape(size, 2 * clades - 2)
    vmem = pl.BlockSpec(memory_space=pltpu.VMEM)
    smem = pl.BlockSpec(memory_space=pltpu.SMEM)
    weighted, mean = pl.pallas_call(
        functools.partial(kernel, (leaves, rates, rows, clades, sites_axis)),
        out_shape=(pltpu.VMEM((piece, 128), jnp.float32), pltpu.VMEM((1, 128), jnp.float32)),
        in_specs=[pl.BlockSpec(memory_space=pltpu.HBM)] * 6,
        out_specs=(vmem, vmem),
        scratch_shapes=[
            pltpu.VMEM((windows, leaves // 8, 64, 128), jnp.int32),
            pltpu.VMEM((size, nodes), jnp.float32),
            pltpu.SMEM((2, leaves - 1), jnp.int32),
            pltpu.VMEM((size, 2 * clades - 2), jnp.float32),
            pltpu.SMEM((2, clades - 1), jnp.int32),
            pltpu.VMEM((clades, piece, 128), jnp.int32),
            pltpu.SemaphoreType.DMA((7,)),
            pltpu.VMEM((leaves * entries, 8, 128), jnp.float32),
            pltpu.VMEM(((leaves - 2) * size, 128), jnp.float32),
            pltpu.VMEM(((2 * clades - 2) * size, 128), jnp.float32),
            pltpu.VMEM((windows, 8 // piece, entries + 1, piece, 128), jnp.float32),
            pltpu.VMEM((2 * clades - 2, entries + 1, piece, 128), jnp.float32),
            pltpu.VMEM((clades * sites_axis, 1, 128), jnp.float32),
            pltpu.SemaphoreType.DMA,
            pltpu.SemaphoreType.DMA,
            pltpu.SemaphoreType.DMA,
            pltpu.SemaphoreType.DMA,
            pltpu.SemaphoreType.REGULAR,
        ] + [pltpu.VMEM((nodes * entries, 8 * width, 128), jnp.float32) for width in [1] * near + [windows - near]],
        compiler_params=pltpu.CompilerParams(
            collective_id=0, has_side_effects=True, vmem_limit_bytes=67043328 - 16384),
    )(codes, matrices, clade_children.T, upper, upper_children.T, pattern_weights.reshape(clades, piece, 128))
    weighted, mean = pl.pallas_call(
        functools.partial(finish, float(sites * sites_axis)),
        out_shape=(jax.ShapeDtypeStruct((piece, 128), jnp.float32), jax.ShapeDtypeStruct((1,), jnp.float32)),
        in_specs=[vmem, vmem],
        out_specs=(pl.BlockSpec(memory_space=pltpu.HBM), smem),
        scratch_shapes=[pltpu.SemaphoreType.DMA],
    )(pltpu.with_memory_space_constraint(weighted, pltpu.VMEM), pltpu.with_memory_space_constraint(mean, pltpu.VMEM))
    return weighted.reshape(sites // clades), mean.reshape(())


def solution(mesh):
    placed = (
        P("clade", "site"),
        P("clade", None, None, None),
        P("clade", None),
        P(),
        P(),
        P("site"),
    )
    return jax.shard_map(
        per_device,
        mesh=mesh,
        in_specs=placed,
        out_specs=(P(("site", "clade")), P()),
        check_vma=False,
    )
```

```python
import functools

import jax
import jax.numpy as jnp
from jax import lax
from jax.experimental import pallas as pl
from jax.experimental.pallas import tpu as pltpu
from jax.sharding import PartitionSpec as P

MESH = pl.DeviceIdType.MESH
EARLY = 10
LAG = 22


def tree_max(values):
    while len(values) > 1:
        paired = [jnp.maximum(a, b) for a, b in zip(values[::2], values[1::2])]
        values = paired + ([values[-1]] if len(values) % 2 else [])
    return values[0]


def tree_sum(values):
    while len(values) > 1:
        paired = [a + b for a, b in zip(values[::2], values[1::2])]
        values = paired + ([values[-1]] if len(values) % 2 else [])
    return values[0]


def look_up(table, code):
    dims = lax.GatherDimensionNumbers(
        offset_dims=(), collapsed_slice_dims=(0,), start_index_map=(0,),
        operand_batching_dims=(1,), start_indices_batching_dims=(1,))
    return lax.gather(table, code[..., None], dims, slice_sizes=(1, 1), mode=lax.GatherScatterMode.PROMISE_IN_BOUNDS)


def kernel(dims, tips_in, matrices_in, children_in, upper_in, upper_children_in, weights_in,
           weighted, mean, tips, matrices, children, upper, upper_children, weights, load,
           tables, branch, upper_branch, root, held, sums,
           root_send, root_recv, sum_send, sum_recv, here, *moved):
    leaves, rates, rows, clades, sites_axis = dims
    entries = rates * 4
    size = entries * 4
    nodes = 2 * leaves - 2
    inner = leaves - 1
    piece = rows // clades
    shares = 8 // piece
    windows = rows // 8
    near = windows // 2
    me = lax.axis_index("clade")
    block = lax.axis_index("site")
    devices = clades * sites_axis
    mine = block * clades + me
    own = me // shares
    my_share = lax.rem(me, shares)
    half, low = own // near, lax.rem(own, near)
    order = [(1 - half) * near + s for s in range(near)]
    order += [half * near + lax.rem(low + s + 1, near) for s in range(near)]
    groups = [[t] for t in range(windows)]

    def tips_start(turn):
        for k in range(leaves // 8):
            pltpu.make_async_copy(tips_in.at[k, pl.ds(order[turn] * 64, 64), :], tips.at[turn, k],
                                  load.at[turn // near]).start()

    def tips_wait(start, stop):
        span = tips.at[pl.ds(start, stop - start)]
        pltpu.make_async_copy(span, span, load.at[start // near]).wait()

    loads = [pltpu.make_async_copy(source, target, load.at[k]) for k, source, target in [
        (2, matrices_in, matrices), (3, children_in, children), (4, upper_in, upper),
        (2, upper_children_in, upper_children), (3, weights_in, weights)]]
    loads[0].start()
    for turn in range(near):
        tips_start(turn)
    for copy in loads[1:3]:
        copy.start()
    for turn in range(near, windows):
        tips_start(turn)

    barrier = pltpu.get_barrier_semaphore()

    def to_site(index):
        return {"site": index // clades, "clade": lax.rem(index, clades)}

    for step in range(1, clades):
        pl.semaphore_signal(barrier, inc=1, device_id={"clade": lax.rem(me + step, clades)}, device_id_type=MESH)

    def greet(other, carry):
        pl.semaphore_signal(barrier, inc=1, device_id=to_site(other), device_id_type=MESH)
        return carry

    lax.fori_loop((block + 1) * clades, devices, greet, 0)

    loads[0].wait()
    loads[3].start()
    first = lax.broadcasted_iota(jnp.int32, (8, 128), 0) < 4

    def lay_out(node):
        branch[node * size:(node + 1) * size, :] = jnp.broadcast_to(
            matrices[:, leaves + node:leaves + node + 1], (size, 128))

    def tip_codes(turn, i):
        return tips[turn, i // 8, pl.ds(lax.rem(i, 8), 8, stride=8), :]

    def tip_rest(i, targets):
        codes = {turn: tip_codes(turn, i) for group in targets for turn in groups[group]}
        for entry in range(entries):
            table = tables[i * entries + entry]
            for group in targets:
                for w, turn in enumerate(groups[group]):
                    moved[group][i * entries + entry, w * 8:(w + 1) * 8, :] = look_up(table, codes[turn])

    def tip_tables(i):
        for pair in range(entries // 2):
            both = jnp.broadcast_to(matrices[pair * 8:pair * 8 + 8, i:i + 1], (8, 128))
            tables[i * entries + 2 * pair] = jnp.where(first, both, 1.0)
            tables[i * entries + 2 * pair + 1] = jnp.where(first, pltpu.roll(both, 4, 0), 1.0)

    for i in range(EARLY):
        tip_tables(i)
    tips_wait(0, near)
    for i in range(leaves):
        if i + EARLY < leaves:
            tip_tables(i + EARLY)
        tip_rest(i, [0, 1])
    loads[1].wait()
    loads[4].start()
    tips_wait(near, windows)
    loads[2].wait()
    for node in range(2 * clades - 2):
        upper_branch[node * size:(node + 1) * size, :] = jnp.broadcast_to(upper[:, node:node + 1], (size, 128))

    def spread(ref, row, count=8):
        return jnp.broadcast_to(ref[pl.ds(row, 1), :], (count, 128))

    def merge(left, right):
        product = [a * b for a, b in zip(left, right)]
        biggest = tree_max(product)
        inverse = 1.0 / biggest
        return [p * inverse for p in product], jnp.log(biggest)

    def transform(ref, base, parts, store):
        count = parts[0][0].shape[0]
        for rate in range(rates):
            for state in range(4):
                entry = rate * 4 + state
                acc = None
                for b in range(4):
                    weight = spread(ref, base + entry * 4 + b, count)
                    terms = [weight * part[rate * 4 + b] for part in parts]
                    acc = terms if acc is None else [x + y for x, y in zip(acc, terms)]
                for w, value in enumerate(acc):
                    store(entry, w, value)

    def rows_of(j):
        return children[0, j] * entries, children[1, j] * entries

    def answer(other, carry):
        pl.semaphore_signal(here, inc=1, device_id={"site": other}, device_id_type=MESH)
        return carry

    class Walk:
        def __init__(self, turn):
            self.turn, self.rows, self.scale = turn, moved[turn], 0.0

        def take(self, j):
            c, d = rows_of(j)
            self.part, log_m = merge([self.rows[c + e] for e in range(entries)],
                                     [self.rows[d + e] for e in range(entries)])
            self.scale = self.scale + log_m

        def put(self, j):
            def store(entry, w, value):
                self.rows[(leaves + j) * entries + entry] = value

            transform(branch, j * size, [self.part], store)

        def finish(self):
            def store(entry, w, value):
                for k in range(shares):
                    root[self.turn, k, entry] = value[k * piece:(k + 1) * piece, :]

            transform(upper_branch, me * size, [self.part], store)
            store(entries, 0, self.scale)
            if self.turn == 0:
                pl.semaphore_wait(barrier, clades - 1 + block * clades)
            for k in range(shares):
                if self.turn < windows - 1:
                    share = k
                elif k:
                    share = lax.rem(my_share + k, shares)
                else:
                    continue
                pltpu.make_async_remote_copy(
                    src_ref=root.at[self.turn, share], dst_ref=held.at[me], send_sem=root_send, recv_sem=root_recv,
                    device_id={"clade": order[self.turn] * shares + share}, device_id_type=MESH).start()

    for pair in range(0, windows, 2):
        ahead, behind = Walk(pair), Walk(pair + 1)
        later = list(range(pair + 2, min(pair + 4, windows)))
        pending = iter(range(leaves))
        for step in range(inner + LAG):
            alone = step >= inner
            if not alone:
                ahead.take(step)
            if 0 < step - LAG:
                behind.put(step - LAG - 1)
            if step < inner - 1:
                if pair == 0:
                    lay_out(step)
                ahead.put(step)
            if step == inner - 1:
                ahead.finish()
            if step >= LAG:
                behind.take(step - LAG)
            if alone and later:
                for i in range(-(-leaves // LAG)):
                    tip = next(pending, None)
                    if tip is not None:
                        tip_rest(tip, later)
        behind.finish()
        if pair == 0:
            lax.fori_loop(0, block, answer, 0)

    held[me] = root[windows - 1, my_share]
    roots = pltpu.make_async_remote_copy(
        src_ref=held.at[pl.ds(0, clades - 1)], dst_ref=held.at[pl.ds(0, clades - 1)],
        send_sem=root_send, recv_sem=root_recv, device_id={"clade": lax.rem(me + 1, clades)}, device_id_type=MESH)
    loads[3].wait()
    loads[4].wait()
    roots.wait_recv()

    scale = tree_sum([held[k, entries] for k in range(clades)])
    for j in range(clades - 1):
        c = upper_children[0, j]
        d = upper_children[1, j]
        part, log_m = merge([held[c, e] for e in range(entries)], [held[d, e] for e in range(entries)])
        scale = scale + log_m
        if j < clades - 2:
            def store_upper(entry, w, value):
                held[clades + j, entry, :, :] = value

            transform(upper_branch, (clades + j) * size, [part], store_upper)
    summed = tree_sum(part) / (4.0 * rates)
    value = weights[me].astype(jnp.float32) * (jnp.log(summed) + scale) / float(leaves * clades)
    weighted[...] = value

    sums[mine] = jnp.sum(value, axis=0, keepdims=True)

    def send_sum(other, carry):
        pltpu.make_async_remote_copy(
            src_ref=sums.at[mine], dst_ref=sums.at[mine], send_sem=sum_send, recv_sem=sum_recv,
            device_id=to_site(other), device_id_type=MESH).start()
        return carry

    lax.fori_loop(0, block * clades, send_sum, 0)
    for step in range(1, clades):
        send_sum(block * clades + lax.rem(me + step, clades), 0)

    @pl.when(block < sites_axis - 1)
    def _():
        pl.semaphore_wait(here, sites_axis - 1 - block)

    lax.fori_loop((block + 1) * clades, devices, send_sum, 0)
    everyone = pltpu.make_async_remote_copy(
        src_ref=sums.at[pl.ds(1, devices - 1)], dst_ref=sums.at[pl.ds(1, devices - 1)],
        send_sem=sum_send, recv_sem=sum_recv, device_id={"clade": lax.rem(me + 1, clades)}, device_id_type=MESH)
    roots.wait_send()
    everyone.wait_send()
    everyone.wait_recv()
    mean[...] = tree_sum([sums[k] for k in range(devices)])


def finish(sites, value, total, weighted, mean, sem):
    copy = pltpu.make_async_copy(value, weighted, sem)
    copy.start()
    mean[0] = jnp.sum(total[...]) / sites
    copy.wait()


def per_device(tips, transition, clade_children, upper_transition, upper_children, pattern_weights):
    leaves, sites = tips.shape
    rates = transition.shape[1]
    clades = lax.axis_size("clade")
    sites_axis = lax.axis_size("site")
    rows = sites // 128
    piece = rows // clades
    windows = rows // 8
    near = windows // 2
    entries = rates * 4
    size = entries * 4
    nodes = 2 * leaves - 2
    codes = tips.reshape(leaves // 8, 8, rows, 128).transpose(0, 2, 1, 3).reshape(leaves // 8, rows * 8, 128)
    matrices = transition.transpose(1, 2, 3, 0).reshape(size, nodes)
    upper = upper_transition.transpose(1, 2, 3, 0).reshape(size, 2 * clades - 2)
    vmem = pl.BlockSpec(memory_space=pltpu.VMEM)
    smem = pl.BlockSpec(memory_space=pltpu.SMEM)
    weighted, mean = pl.pallas_call(
        functools.partial(kernel, (leaves, rates, rows, clades, sites_axis)),
        out_shape=(pltpu.VMEM((piece, 128), jnp.float32), pltpu.VMEM((1, 128), jnp.float32)),
        in_specs=[pl.BlockSpec(memory_space=pltpu.HBM)] * 6,
        out_specs=(vmem, vmem),
        scratch_shapes=[
            pltpu.VMEM((windows, leaves // 8, 64, 128), jnp.int32),
            pltpu.VMEM((size, nodes), jnp.float32),
            pltpu.SMEM((2, leaves - 1), jnp.int32),
            pltpu.VMEM((size, 2 * clades - 2), jnp.float32),
            pltpu.SMEM((2, clades - 1), jnp.int32),
            pltpu.VMEM((clades, piece, 128), jnp.int32),
            pltpu.SemaphoreType.DMA((5,)),
            pltpu.VMEM((leaves * entries, 8, 128), jnp.float32),
            pltpu.VMEM(((leaves - 2) * size, 128), jnp.float32),
            pltpu.VMEM(((2 * clades - 2) * size, 128), jnp.float32),
            pltpu.VMEM((windows, 8 // piece, entries + 1, piece, 128), jnp.float32),
            pltpu.VMEM((2 * clades - 2, entries + 1, piece, 128), jnp.float32),
            pltpu.VMEM((clades * sites_axis, 1, 128), jnp.float32),
            pltpu.SemaphoreType.DMA,
            pltpu.SemaphoreType.DMA,
            pltpu.SemaphoreType.DMA,
            pltpu.SemaphoreType.DMA,
            pltpu.SemaphoreType.REGULAR,
        ] + [pltpu.VMEM((nodes * entries, 8, 128), jnp.float32) for _ in range(windows)],
        compiler_params=pltpu.CompilerParams(
            collective_id=0, has_side_effects=True, vmem_limit_bytes=67043328 - 16384),
    )(codes, matrices, clade_children.T, upper, upper_children.T, pattern_weights.reshape(clades, piece, 128))
    weighted, mean = pl.pallas_call(
        functools.partial(finish, float(sites * sites_axis)),
        out_shape=(jax.ShapeDtypeStruct((piece, 128), jnp.float32), jax.ShapeDtypeStruct((1,), jnp.float32)),
        in_specs=[vmem, vmem],
        out_specs=(pl.BlockSpec(memory_space=pltpu.HBM), smem),
        scratch_shapes=[pltpu.SemaphoreType.DMA],
    )(pltpu.with_memory_space_constraint(weighted, pltpu.VMEM), pltpu.with_memory_space_constraint(mean, pltpu.VMEM))
    return weighted.reshape(sites // clades), mean.reshape(())


def solution(mesh):
    placed = (
        P("clade", "site"),
        P("clade", None, None, None),
        P("clade", None),
        P(),
        P(),
        P("site"),
    )
    return jax.shard_map(
        per_device,
        mesh=mesh,
        in_specs=placed,
        out_specs=(P(("site", "clade")), P()),
        check_vma=False,
    )
```
